32 devices in a mesh: seq: 8 (over y, x, core), head: 4 (over z).
Axes of the slice: x: 2, y: 2, z: 4, core: 2. Of those that a mesh axis runs over, the one named last changes fastest.
Arguments:
- queries: bfloat16 [2048, 2048], P('seq', 'head'), may hold values from -6 to 6
- key_vectors: bfloat16 [2048, 2048], P('seq', 'head'), may hold values from -6 to 6
- value_vectors: bfloat16 [2048, 4096], P('seq', 'head'), may hold values from -8 to 8
- out_weight: bfloat16 [4096, 4096], P('head'), may hold values from -0.125 to 0.125
Outputs:
- mixed: bfloat16 [2048, 4096], P('seq', 'head')
The draws below stay inside these ranges and needn't reach their ends.
All inputs are finite; a program needn't handle non-finite values.
Results may differ from the reference program's by a relative error of at most 0.008.
Values may be sent and summed in bfloat16 or wider, within the bound.
No kernel may reach another device: no remote copies, remote signals or barrier semaphores. Data moves between devices by JAX's collectives and lax.ppermute only.
A program may use at most 256 MiB of HBM per device.

```python
import math
import jax
import jax.numpy as jnp
import numpy as np
from jax import lax

D = 4096
HEADS = 32
KD = 64
VD = 128
FEAT = 2176
TOK_DEV = 256
TOKENS = 2048


def block_draw(key, width, offset_scale, bound):
    first_key, second_key = jax.random.split(key, 2)
    blocks = TOKENS // TOK_DEV
    offsets = offset_scale * jax.random.normal(second_key, (blocks, width), jnp.float32)
    noise = jax.random.normal(first_key, (TOKENS, width), jnp.float32)
    values = noise + jnp.repeat(offsets, TOK_DEV, axis=0)
    return jnp.clip(values, -bound, bound)


def draw_key_vectors(key, part):
    return block_draw(jax.random.fold_in(key, 11), HEADS * KD, 0.8, 6.0).astype(jnp.bfloat16)


def draw_value_vectors(key, part):
    noise_key = jax.random.fold_in(key, 23)
    values = jnp.clip(3.0 * jax.random.normal(noise_key, (TOKENS, HEADS * VD), jnp.float32), -8.0, 8.0)
    return values.astype(jnp.bfloat16)


def raised(values, rng, source, target, shards_of, factor):
    owner, partner = [(jnp.arange(values.shape[axis_at]) // (values.shape[axis_at] // shards_of)).reshape([-1 if axis == axis_at else 1 for axis in range(values.ndim)]) for axis_at in (source, target)]
    chosen = jax.random.permutation(rng, shards_of)[partner]
    strong = (owner == chosen) | (owner == (partner + shards_of // 2) % shards_of)
    return jnp.where(strong, factor * values, values)


def level_of(own_key, shape, pieces, smallest, high):
    loudness, own = 1.0, jax.random.fold_in(own_key, 6)
    for position, blocks in pieces:
        draws = jnp.exp(jax.random.uniform(jax.random.fold_in(own, position), (blocks,), jnp.float32, smallest / len(pieces), high / len(pieces)))
        loudness = loudness * jnp.repeat(draws, shape[position] // blocks).reshape([-1 if axis == position else 1 for axis in range(len(shape))])
    return loudness


def centred(stream_key, extent, spread, limit, cuts=(), kind=jnp.bfloat16):
    values = jax.random.normal(stream_key, extent, jnp.float32) * spread
    if len(cuts) > 0:
        values = level_of(stream_key, extent, cuts, -0.22, 0.18) * values
    return jnp.clip(values, min=-limit, max=limit).astype(kind)


def noise_with(own_key, extent, scale, reach, shards, heavy, kind=jnp.bfloat16):
    values = scale * jax.random.normal(own_key, extent, jnp.float32)
    if shards:
        values = values * level_of(own_key, extent, shards, -0.22, 0.18)
    return jnp.clip(raised(values, jax.random.fold_in(own_key, 3), *heavy), -reach, reach).astype(kind)


def setup_inputs(seed: int = 0) -> dict:
    keys = jax.random.split(jax.random.key(seed), 5)
    queries = centred(keys[0], (TOKENS, HEADS * KD), 1.0, 6.0, ((0, 8), (1, 4)))
    key_vectors = draw_key_vectors(jax.random.fold_in(keys[4], 71), 0)
    value_vectors = draw_value_vectors(jax.random.fold_in(keys[4], 71), 0)
    out_weight = noise_with(keys[3], (HEADS * VD, D), (HEADS * VD) ** -0.5, 0.125, ((0, 4),), (0, 1, 4, 2.0))
    return {"queries": queries, "key_vectors": key_vectors, "value_vectors": value_vectors, "out_weight": out_weight}


def feature_tables(key_dim, width):
    left_index = [0]
    right_index = [0]
    scales = [1.0]
    for outer_i in range(key_dim):
        left_index.append(0)
        right_index.append(outer_i + 1)
        scales.append(1.0)
    for outer_i in range(key_dim):
        for inner_j in range(outer_i, key_dim):
            left_index.append(outer_i + 1)
            right_index.append(inner_j + 1)
            scales.append(math.sqrt(0.5) if outer_i == inner_j else 1.0)
    while len(scales) < width:
        left_index.append(key_dim + 1)
        right_index.append(key_dim + 1)
        scales.append(0.0)
    return (np.array(left_index, np.int32), np.array(right_index, np.int32), np.array(scales, np.float32))

def features(vectors, key_dim, width):
    left_index, right_index, scales = feature_tables(key_dim, width)
    scaled = vectors.astype(jnp.float32) * key_dim ** (-0.25)
    unit_column = jnp.ones(scaled.shape[:-1] + (1,), jnp.float32)
    padded = jnp.concatenate([unit_column, scaled, jnp.zeros_like(unit_column)], axis=-1)
    product = jnp.take(padded, left_index, axis=-1) * jnp.take(padded, right_index, axis=-1)
    return (product * jnp.asarray(scales, jnp.float32)).astype(jnp.bfloat16)

def rounded(values):
    return lax.optimization_barrier(values.astype(jnp.bfloat16)).astype(jnp.float32)

def reference(queries, key_vectors, value_vectors, out_weight):
    slabs = TOKENS // TOK_DEV
    q_all = queries.reshape(slabs, TOK_DEV, HEADS, KD)
    k_all = key_vectors.reshape(slabs, TOK_DEV, HEADS, KD)
    v_all = value_vectors.reshape(slabs, TOK_DEV, HEADS, VD)
    positions = jnp.arange(TOK_DEV, dtype=jnp.int32)
    causal = positions[None, :] <= positions[:, None]
    high = lax.Precision.HIGHEST

    def advance(carried, slab):
        states, norms = carried
        q_heads, k_heads, v_heads = slab
        phi_q = lax.optimization_barrier(features(q_heads, KD, FEAT)).astype(jnp.float32)
        phi_k = lax.optimization_barrier(features(k_heads, KD, FEAT)).astype(jnp.float32)
        v_float = v_heads.astype(jnp.float32)
        scores = jnp.einsum('bhd,thd->hbt', q_heads.astype(jnp.float32), k_heads.astype(jnp.float32), precision=high) * KD ** (-0.5)
        weights = jnp.where(causal[None], 1.0 + scores + 0.5 * scores * scores, 0.0)
        weights = rounded(weights)
        numer = jnp.einsum('hbt,thc->bhc', weights, v_float, precision=high)
        denom = lax.optimization_barrier(jnp.sum(weights, axis=-1)).T
        prior = rounded(states)
        prior_norm = rounded(norms)
        numer = numer + jnp.einsum('bhf,hfc->bhc', phi_q, prior, precision=high)
        denom = denom + jnp.einsum('bhf,hf->bh', phi_q, prior_norm, precision=high)
        result = (numer / denom[..., None]).astype(jnp.bfloat16).reshape(TOK_DEV, HEADS * VD)
        states = states + jnp.einsum('thf,thc->hfc', phi_k, v_float, precision=high)
        norms = norms + lax.optimization_barrier(jnp.sum(phi_k, axis=0))
        return ((states, norms), result)
    start = (jnp.zeros((HEADS, FEAT, VD), jnp.float32), jnp.zeros((HEADS, FEAT), jnp.float32))
    carried, results = lax.scan(advance, start, (q_all, k_all, v_all))
    attention = results.reshape(TOKENS, HEADS * VD)
    return jnp.dot(attention, out_weight, preferred_element_type=jnp.float32).astype(jnp.bfloat16)
```

```python
import functools
import math

import jax
import jax.numpy as jnp
from jax import lax
from jax.experimental import pallas as pl
from jax.experimental.pallas import tpu as pltpu
from jax.sharding import PartitionSpec as P

KD = 64
VD = 128


def swap(value, axis, bits):
    count = lax.axis_size(axis)
    return lax.ppermute(value, axis, [(i, i ^ bits) for i in range(count)])


def pack_kernel(place, q_ref, k_ref, v_ref, *outs):
    wide_k = outs[0].shape[1] // 4
    wide_v = 2 * wide_k
    for turn, out in enumerate(outs):
        chip = place[0] ^ turn
        at_k = pl.multiple_of(chip * wide_k, wide_k)
        at_v = pl.multiple_of(chip * wide_v, wide_v)
        out[:, :wide_k] = q_ref[:, pl.ds(at_k, wide_k)]
        out[:, wide_k:wide_v] = k_ref[:, pl.ds(at_k, wide_k)]
        out[:, wide_v:] = v_ref[:, pl.ds(at_v, wide_v)]


def pack(place, queries, keys, values, chips):
    length, width = queries.shape
    each = jax.ShapeDtypeStruct((length, 4 * width // chips), queries.dtype)
    return pl.pallas_call(
        pack_kernel,
        out_shape=(each,) * chips,
        in_specs=[pl.BlockSpec(memory_space=pltpu.SMEM)] + [pl.BlockSpec(memory_space=pltpu.VMEM)] * 3,
        name="pack",
    )(place, queries, keys, values)


def attend_kernel(place, *refs, chips, heads):
    mine, partner = refs[:chips], refs[chips : 2 * chips]
    outs = refs[2 * chips : 3 * chips]
    q_all, k_all, v_all, o_all = refs[3 * chips :]
    length = mine[0].shape[0]
    wide_k, wide_v = heads * KD, heads * VD
    chip, core = place[0], place[1]
    ones = jnp.ones((length, VD), jnp.bfloat16)
    for turn in range(chips):
        there = chip ^ turn
        q_all[pl.ds(pl.multiple_of(there * length, length), length), :] = mine[turn][:, :wide_k]
        for ref, side in ((mine[turn], core), (partner[turn], 1 - core)):
            rows = pl.ds(pl.multiple_of((2 * there + side) * length, length), length)
            k_all[rows, :] = ref[:, wide_k : 2 * wide_k]
            for head in range(heads):
                at = 2 * wide_k + head * VD
                v_all[rows, 2 * head * VD : (2 * head + 1) * VD] = ref[:, at : at + VD]
                v_all[rows, (2 * head + 1) * VD : (2 * head + 2) * VD] = ones
    row = lax.broadcasted_iota(jnp.int32, (length, 2 * length), 0) + core * length
    seen = lax.broadcasted_iota(jnp.int32, (length, 2 * length), 1) <= row
    lane = lax.broadcasted_iota(jnp.int32, (length, wide_k), 1) // KD
    for index in range(chips):
        q = q_all[index * length : (index + 1) * length, :] * jnp.bfloat16(KD ** (-0.5))
        for head in range(heads):
            own = jnp.where(lane == head, q, jnp.bfloat16(0))
            columns = slice(2 * head * VD, (2 * head + 2) * VD)
            total = None
            for block in range(index + 1):
                rows = slice(2 * block * length, 2 * (block + 1) * length)
                scores = lax.dot_general(
                    own, k_all[rows, :], (((1,), (1,)), ((), ())), preferred_element_type=jnp.float32
                )
                raised = scores + 1.0
                weights = raised * raised + 1.0
                if block == index:
                    weights = jnp.where(seen, weights, 0.0)
                part = jnp.dot(
                    weights.astype(jnp.bfloat16), v_all[rows, columns], preferred_element_type=jnp.float32
                )
                total = part if total is None else total + part
            o_all[index * length : (index + 1) * length, head * VD : (head + 1) * VD] = (
                total[:, :VD] / total[:, VD:]
            ).astype(jnp.bfloat16)
    for turn, out in enumerate(outs):
        out[...] = o_all[pl.ds(pl.multiple_of((chip ^ turn) * length, length), length), :]


def attend(place, mine, partner, heads):
    chips, (length, _) = len(mine), mine[0].shape
    each = jax.ShapeDtypeStruct((length, heads * VD), jnp.bfloat16)
    whole = 2 * chips * length
    return pl.pallas_call(
        functools.partial(attend_kernel, chips=chips, heads=heads),
        out_shape=(each,) * chips,
        in_specs=[pl.BlockSpec(memory_space=pltpu.SMEM)] + [pl.BlockSpec(memory_space=pltpu.VMEM)] * (2 * chips),
        scratch_shapes=[
            pltpu.VMEM((whole // 2, heads * KD), jnp.bfloat16),
            pltpu.VMEM((whole, heads * KD), jnp.bfloat16),
            pltpu.VMEM((whole, 2 * heads * VD), jnp.bfloat16),
            pltpu.VMEM((whole // 2, heads * VD), jnp.bfloat16),
        ],
        name="attend",
    )(place, *mine, *partner)


def project_kernel(place, *refs, chips):
    pieces, (w_ref, out) = refs[:chips], refs[chips:]
    depth = pieces[0].shape[1]
    total = None
    for turn in range(chips):
        rows = pl.ds(pl.multiple_of((place[0] ^ turn) * depth, depth), depth)
        part = jnp.dot(pieces[turn][...], w_ref[rows, :], preferred_element_type=jnp.float32)
        total = part if total is None else total + part
    out[...] = total.astype(out.dtype)


def project(place, pieces, weight, slot, columns, dtype):
    chips, (length, depth) = len(pieces), pieces[0].shape
    rows = weight.shape[0]
    return pl.pallas_call(
        functools.partial(project_kernel, chips=chips),
        grid_spec=pltpu.PrefetchScalarGridSpec(
            num_scalar_prefetch=1,
            grid=(1,),
            in_specs=[pl.BlockSpec((length, depth), lambda i, place: (0, 0))] * chips
            + [pl.BlockSpec((rows, columns), lambda i, place: (0, place[2 + slot]))],
            out_specs=pl.BlockSpec((length, columns), lambda i, place: (0, 0)),
        ),
        out_shape=jax.ShapeDtypeStruct((length, columns), dtype),
        name=f"project{slot}",
    )(place, *pieces, weight)


def exchanged(queries, key_vectors, value_vectors, out_weight):
    seq, ranks = lax.axis_size("seq"), lax.axis_size("head")
    chips = seq // 2
    heads = out_weight.shape[0] // VD // chips
    here, rank = lax.axis_index("seq"), lax.axis_index("head")
    columns = out_weight.shape[1] // ranks
    order = jnp.asarray([[3, 2, 1, 0], [3, 2, 0, 1], [0, 1, 3, 2], [0, 1, 2, 3]], jnp.int32)[rank]
    place = jnp.concatenate([jnp.stack([here >> 1, here & 1]).astype(jnp.int32), order])

    packed = pack(place, queries, key_vectors, value_vectors, chips)
    mine = [packed[0]] + [swap(packed[turn], "seq", 2 * turn) for turn in range(1, chips)]
    partner = [swap(piece, "seq", 1) for piece in mine]
    outs = attend(place, mine, partner, heads)
    pieces = [outs[0]] + [swap(outs[turn], "seq", 2 * turn) for turn in range(1, chips)]

    def hop(value, source, target):
        return lax.ppermute(value, "head", [(source, target), (ranks - 1 - source, ranks - 1 - target)])

    bf16, f32 = jnp.bfloat16, jnp.float32
    parts = [project(place, pieces, out_weight, slot, columns, bf16) for slot in range(3)]
    own = project(place, pieces, out_weight, 3, columns, f32)
    first = hop(parts[0], 0, 1)
    second = hop(parts[1], 0, 1)
    third = hop(parts[2], 0, 1)
    middle = hop((parts[0].astype(f32) + first.astype(f32)).astype(bf16), 1, 2)
    late = hop((parts[1].astype(f32) + second.astype(f32)).astype(bf16), 1, 2)
    last = hop((parts[2].astype(f32) + middle.astype(f32)).astype(bf16), 2, 3)
    total = own + third.astype(f32) + late.astype(f32) + last.astype(f32)
    return total.astype(bf16)


def gathered(queries, key_vectors, value_vectors, out_weight):
    heads_here = out_weight.shape[0] // VD
    length = queries.shape[0]
    here = lax.axis_index("seq")
    k_all = lax.all_gather(key_vectors, "seq", axis=0, tiled=True)
    v_all = lax.all_gather(value_vectors, "seq", axis=0, tiled=True)
    rows = here * length + jnp.arange(length, dtype=jnp.int32)
    causal = jnp.arange(k_all.shape[0], dtype=jnp.int32)[None, :] <= rows[:, None]
    results = []
    for head in range(heads_here):
        q = queries[:, head * KD : (head + 1) * KD]
        k = k_all[:, head * KD : (head + 1) * KD]
        v = v_all[:, head * VD : (head + 1) * VD]
        scores = jnp.einsum("bd,td->bt", q, k, preferred_element_type=jnp.float32) * KD ** (-0.5)
        weights = jnp.where(causal, 1.0 + scores + 0.5 * scores * scores, 0.0).astype(jnp.bfloat16)
        numer = jnp.dot(weights, v, preferred_element_type=jnp.float32)
        denom = jnp.sum(weights, axis=-1, dtype=jnp.float32)
        results.append((numer / denom[:, None]).astype(jnp.bfloat16))
    attention = jnp.concatenate(results, axis=1)
    partial = jnp.dot(attention, out_weight, preferred_element_type=jnp.float32)
    mixed = lax.psum_scatter(partial, "head", scatter_dimension=1, tiled=True)
    return mixed.astype(jnp.bfloat16)


def per_device(queries, key_vectors, value_vectors, out_weight):
    seq, ranks = lax.axis_size("seq"), lax.axis_size("head")
    heads_here = out_weight.shape[0] // VD
    chips = seq // 2
    paired = seq == 2 * chips and chips > 0 and chips & (chips - 1) == 0
    if paired and ranks == 4 and heads_here % chips == 0 and (heads_here // chips * KD) % 128 == 0:
        return exchanged(queries, key_vectors, value_vectors, out_weight)
    return gathered(queries, key_vectors, value_vectors, out_weight)


def solution(mesh):
    placed = (P("seq", "head"), P("seq", "head"), P("seq", "head"), P("head", None))
    return jax.shard_map(
        per_device, mesh=mesh, in_specs=placed, out_specs=P("seq", "head"), check_vma=False
    )
```

```python
import functools
import math

import jax
import jax.numpy as jnp
from jax import lax
from jax.experimental import pallas as pl
from jax.experimental.pallas import tpu as pltpu
from jax.sharding import PartitionSpec as P

KD = 64
VD = 128


def swap(value, axis, bits):
    count = lax.axis_size(axis)
    return lax.ppermute(value, axis, [(i, i ^ bits) for i in range(count)])


def in_vmem(*values):
    return [pltpu.with_memory_space_constraint(value, pltpu.VMEM) for value in values]


def in_hbm(*values):
    return [pltpu.with_memory_space_constraint(value, pltpu.HBM) for value in values]


def room(mebibytes):
    return pltpu.CompilerParams(vmem_limit_bytes=mebibytes << 20)


def seat():
    here = lax.axis_index("seq")
    return here >> 1, here & 1


def pack_kernel(q_ref, k_ref, v_ref, *refs):
    outs, arrived = refs[:-1], refs[-1]
    wide_k = outs[0].shape[1] // 4
    here, _ = seat()
    copies = []
    for turn in (*range(1, len(outs)), 0):
        at = 0
        for source, wide in ((q_ref, wide_k), (k_ref, wide_k), (v_ref, 2 * wide_k)):
            columns = pl.ds(pl.multiple_of((here ^ turn) * wide, wide), wide)
            copies.append(
                pltpu.make_async_copy(
                    source.at[:, columns], outs[turn].at[:, at : at + wide], arrived.at[len(copies)]
                )
            )
            at += wide
    for copy in copies:
        copy.start()
    for copy in copies:
        copy.wait()


def pack(queries, keys, values, chips):
    length, width = queries.shape
    each = pltpu.VMEM((length, 4 * width // chips), queries.dtype)
    return pl.pallas_call(
        pack_kernel,
        out_shape=(each,) * chips,
        in_specs=[pl.BlockSpec(memory_space=pltpu.HBM)] * 3,
        scratch_shapes=[pltpu.SemaphoreType.DMA((3 * chips,))],
        compiler_params=room(8),
        name="pack",
    )(*in_hbm(queries, keys, values))


def attend_kernel(*refs, chips, heads):
    mine, partner, w_ref = refs[:chips], refs[chips : 2 * chips], refs[2 * chips]
    outs, w_out = refs[2 * chips + 1 : 3 * chips + 1], refs[3 * chips + 1]
    q_all, k_all, v_all, o_all, arrived = refs[3 * chips + 2 :]
    fetch = pltpu.make_async_copy(w_ref, w_out, arrived.at[0])
    fetch.start()
    length = mine[0].shape[0]
    wide_k = heads * KD
    chip, core = seat()
    ones = jnp.ones((length, VD), jnp.bfloat16)
    for turn in range(chips):
        there = chip ^ turn
        q_all[pl.ds(pl.multiple_of(there * length, length), length), :] = mine[turn][:, :wide_k]
        for ref, side in ((mine[turn], core), (partner[turn], 1 - core)):
            rows = pl.ds(pl.multiple_of((2 * there + side) * length, length), length)
            k_all[rows, :] = ref[:, wide_k : 2 * wide_k]
            for head in range(heads):
                at = 2 * wide_k + head * VD
                v_all[rows, 2 * head * VD : (2 * head + 1) * VD] = ref[:, at : at + VD]
                v_all[rows, (2 * head + 1) * VD : (2 * head + 2) * VD] = ones
    row = lax.broadcasted_iota(jnp.int32, (length, 2 * length), 0) + core * length
    seen = lax.broadcasted_iota(jnp.int32, (length, 2 * length), 1) <= row
    lane = lax.broadcasted_iota(jnp.int32, (length, wide_k), 1) // KD
    for index in range(chips):
        q = q_all[index * length : (index + 1) * length, :] * jnp.bfloat16(KD ** (-0.5))
        for head in range(heads):
            own = jnp.where(lane == head, q, jnp.bfloat16(0))
            columns = slice(2 * head * VD, (2 * head + 2) * VD)
            total = None
            for block in range(index + 1):
                rows = slice(2 * block * length, 2 * (block + 1) * length)
                scores = lax.dot_general(
                    own, k_all[rows, :], (((1,), (1,)), ((), ())), preferred_element_type=jnp.float32
                )
                raised = scores + 1.0
                weights = raised * raised + 1.0
                if block == index:
                    weights = jnp.where(seen, weights, 0.0)
                part = jnp.dot(
                    weights.astype(jnp.bfloat16), v_all[rows, columns], preferred_element_type=jnp.float32
                )
                total = part if total is None else total + part
            o_all[index * length : (index + 1) * length, head * VD : (head + 1) * VD] = (
                total[:, :VD] / total[:, VD:]
            ).astype(jnp.bfloat16)
    for turn, out in enumerate(outs):
        out[...] = o_all[pl.ds(pl.multiple_of((chip ^ turn) * length, length), length), :]
    fetch.wait()


def attend(mine, partner, weight, heads):
    chips, (length, _) = len(mine), mine[0].shape
    each = pltpu.VMEM((length, heads * VD), jnp.bfloat16)
    whole = 2 * chips * length
    return pl.pallas_call(
        functools.partial(attend_kernel, chips=chips, heads=heads),
        out_shape=(*(each,) * chips, pltpu.VMEM(weight.shape, weight.dtype)),
        in_specs=[pl.BlockSpec(memory_space=pltpu.VMEM)] * (2 * chips) + [pl.BlockSpec(memory_space=pltpu.HBM)],
        scratch_shapes=[
            pltpu.VMEM((whole // 2, heads * KD), jnp.bfloat16),
            pltpu.VMEM((whole, heads * KD), jnp.bfloat16),
            pltpu.VMEM((whole, 2 * heads * VD), jnp.bfloat16),
            pltpu.VMEM((whole // 2, heads * VD), jnp.bfloat16),
            pltpu.SemaphoreType.DMA((1,)),
        ],
        compiler_params=room(24),
        name="attend",
    )(*in_vmem(*mine, *partner), *in_hbm(weight))


def block_at(slot):
    rank = lax.axis_index("head")
    turns = [(3, 3, 0, 0), (2, 2, 1, 1), (1, 0, 3, 2), (0, 1, 2, 3)][slot]
    block = jnp.int32(turns[0])
    for other in range(1, 4):
        block = jnp.where(rank == other, jnp.int32(turns[other]), block)
    return block


def project_kernel(*refs, chips, slots):
    pieces, w_ref, outs = refs[:chips], refs[chips], refs[chips + 1 :]
    depth = pieces[0].shape[1]
    columns = outs[0].shape[1]
    here, _ = seat()
    for slot, out in zip(slots, outs):
        at = pl.ds(pl.multiple_of(block_at(slot) * columns, columns), columns)
        total = None
        for turn in range(chips):
            rows = pl.ds(pl.multiple_of((here ^ turn) * depth, depth), depth)
            part = jnp.dot(pieces[turn][...], w_ref[rows, at], preferred_element_type=jnp.float32)
            total = part if total is None else total + part
        out[...] = total.astype(out.dtype)


def project(pieces, weight, slots, columns, dtypes):
    length = pieces[0].shape[0]
    return pl.pallas_call(
        functools.partial(project_kernel, chips=len(pieces), slots=slots),
        out_shape=tuple(pltpu.VMEM((length, columns), dtype) for dtype in dtypes),
        compiler_params=room(16),
        name="project",
    )(*in_vmem(*pieces, weight))


def exchanged(queries, key_vectors, value_vectors, out_weight):
    seq, ranks = lax.axis_size("seq"), lax.axis_size("head")
    chips = seq // 2
    heads = out_weight.shape[0] // VD // chips
    columns = out_weight.shape[1] // ranks

    packed = pack(queries, key_vectors, value_vectors, chips)
    mine = [packed[0]] + [swap(packed[turn], "seq", 2 * turn) for turn in range(1, chips)]
    partner = [swap(piece, "seq", 1) for piece in mine]
    *outs, weight = attend(mine, partner, out_weight, heads)
    pieces = [outs[0]] + [swap(outs[turn], "seq", 2 * turn) for turn in range(1, chips)]

    def hop(value, source, target):
        return lax.ppermute(value, "head", [(source, target), (ranks - 1 - source, ranks - 1 - target)])

    bf16, f32 = jnp.bfloat16, jnp.float32
    (to_first,) = project(pieces, weight, (0,), columns, (bf16,))
    to_second, to_third, own = project(pieces, weight, (1, 2, 3), columns, (bf16, bf16, f32))
    first = hop(to_first, 0, 1)
    second = hop(to_second, 0, 1)
    third = hop(to_third, 0, 1)
    middle = hop((to_first.astype(f32) + first.astype(f32)).astype(bf16), 1, 2)
    late = hop((to_second.astype(f32) + second.astype(f32)).astype(bf16), 1, 2)
    last = hop((to_third.astype(f32) + middle.astype(f32)).astype(bf16), 2, 3)
    total = own + third.astype(f32) + late.astype(f32) + last.astype(f32)
    return total.astype(bf16)


def gathered(queries, key_vectors, value_vectors, out_weight):
    heads_here = out_weight.shape[0] // VD
    length = queries.shape[0]
    here = lax.axis_index("seq")
    k_all = lax.all_gather(key_vectors, "seq", axis=0, tiled=True)
    v_all = lax.all_gather(value_vectors, "seq", axis=0, tiled=True)
    rows = here * length + jnp.arange(length, dtype=jnp.int32)
    causal = jnp.arange(k_all.shape[0], dtype=jnp.int32)[None, :] <= rows[:, None]
    results = []
    for head in range(heads_here):
        q = queries[:, head * KD : (head + 1) * KD]
        k = k_all[:, head * KD : (head + 1) * KD]
        v = v_all[:, head * VD : (head + 1) * VD]
        scores = jnp.einsum("bd,td->bt", q, k, preferred_element_type=jnp.float32) * KD ** (-0.5)
        weights = jnp.where(causal, 1.0 + scores + 0.5 * scores * scores, 0.0).astype(jnp.bfloat16)
        numer = jnp.dot(weights, v, preferred_element_type=jnp.float32)
        denom = jnp.sum(weights, axis=-1, dtype=jnp.float32)
        results.append((numer / denom[:, None]).astype(jnp.bfloat16))
    attention = jnp.concatenate(results, axis=1)
    partial = jnp.dot(attention, out_weight, preferred_element_type=jnp.float32)
    mixed = lax.psum_scatter(partial, "head", scatter_dimension=1, tiled=True)
    return mixed.astype(jnp.bfloat16)


def per_device(queries, key_vectors, value_vectors, out_weight):
    seq, ranks = lax.axis_size("seq"), lax.axis_size("head")
    heads_here = out_weight.shape[0] // VD
    chips = seq // 2
    paired = seq == 2 * chips and chips > 0 and chips & (chips - 1) == 0
    if paired and ranks == 4 and heads_here % chips == 0 and (heads_here // chips * KD) % 128 == 0:
        return exchanged(queries, key_vectors, value_vectors, out_weight)
    return gathered(queries, key_vectors, value_vectors, out_weight)


def solution(mesh):
    placed = (P("seq", "head"), P("seq", "head"), P("seq", "head"), P("head", None))
    return jax.shard_map(
        per_device, mesh=mesh, in_specs=placed, out_specs=P("seq", "head"), check_vma=False
    )
```

```python
import functools

import jax
import jax.numpy as jnp
from jax import lax
from jax.experimental import pallas as pl
from jax.experimental.pallas import tpu as pltpu
from jax.sharding import PartitionSpec as P


KD = 64
VD = 128


def swap(value, axis, bits):
    count = lax.axis_size(axis)
    return lax.ppermute(value, axis, [(i, i ^ bits) for i in range(count)])


def in_vmem(*values):
    return [pltpu.with_memory_space_constraint(value, pltpu.VMEM) for value in values]


def in_hbm(*values):
    return [pltpu.with_memory_space_constraint(value, pltpu.HBM) for value in values]


def room(mebibytes):
    return pltpu.CompilerParams(vmem_limit_bytes=mebibytes << 20)


def seat():
    here = lax.axis_index("seq")
    return here >> 1, here & 1


def pack_kernel(q_ref, k_ref, v_ref, *refs):
    outs, arrived = refs[:-1], refs[-1]
    wide_k = outs[0].shape[1] // 4
    here, _ = seat()
    copies = []
    for turn in (*range(1, len(outs)), 0):
        at = 0
        for source, wide in ((q_ref, wide_k), (k_ref, wide_k), (v_ref, 2 * wide_k)):
            columns = pl.ds(pl.multiple_of((here ^ turn) * wide, wide), wide)
            copies.append(
                pltpu.make_async_copy(
                    source.at[:, columns], outs[turn].at[:, at : at + wide], arrived.at[len(copies)]
                )
            )
            at += wide
    for copy in copies:
        copy.start()
    for copy in copies:
        copy.wait()


def pack(queries, keys, values, chips):
    length, width = queries.shape
    each = pltpu.VMEM((length, 4 * width // chips), queries.dtype)
    return pl.pallas_call(
        pack_kernel,
        out_shape=(each,) * chips,
        in_specs=[pl.BlockSpec(memory_space=pltpu.HBM)] * 3,
        scratch_shapes=[pltpu.SemaphoreType.DMA((3 * chips,))],
        compiler_params=room(8),
        name="pack",
    )(*in_hbm(queries, keys, values))


def stage_kernel(w_ref, out, arrived):
    copy = pltpu.make_async_copy(w_ref, out, arrived.at[0])
    copy.start()
    copy.wait()


def stage(weight):
    return pl.pallas_call(
        stage_kernel,
        out_shape=pltpu.VMEM(weight.shape, weight.dtype),
        in_specs=[pl.BlockSpec(memory_space=pltpu.HBM)],
        scratch_shapes=[pltpu.SemaphoreType.DMA((1,))],
        compiler_params=room(4),
        name="stage",
    )(*in_hbm(weight))


def attend_rows(q_all, k_all, v_all, o_all, rows_from, core, chips, heads):
    length, wide_k = k_all.shape[0] // (2 * chips), heads * KD
    count = o_all.shape[0] // chips
    row = lax.broadcasted_iota(jnp.int32, (count, 2 * length), 0) + (core * length + rows_from)
    seen = lax.broadcasted_iota(jnp.int32, (count, 2 * length), 1) <= row
    lane = lax.broadcasted_iota(jnp.int32, (count, wide_k), 1) // KD
    for index in range(chips):
        at = index * length + rows_from
        q = q_all[at : at + count, :] * jnp.bfloat16(KD ** (-0.5))
        for head in range(heads):
            own = jnp.where(lane == head, q, jnp.bfloat16(0))
            columns = slice(2 * head * VD, (2 * head + 2) * VD)
            total = None
            for block in range(index + 1):
                rows = slice(2 * block * length, 2 * (block + 1) * length)
                scores = lax.dot_general(
                    own, k_all[rows, :], (((1,), (1,)), ((), ())), preferred_element_type=jnp.float32
                )
                raised = scores + 1.0
                weights = raised * raised + 1.0
                if block == index:
                    weights = jnp.where(seen, weights, 0.0)
                part = jnp.dot(
                    weights.astype(jnp.bfloat16), v_all[rows, columns], preferred_element_type=jnp.float32
                )
                total = part if total is None else total + part
            o_all[index * count : (index + 1) * count, head * VD : (head + 1) * VD] = (
                total[:, :VD] / total[:, VD:]
            ).astype(jnp.bfloat16)


def deal(o_all, outs, chip):
    count = outs[0].shape[0]
    for turn, out in enumerate(outs):
        out[...] = o_all[pl.ds(pl.multiple_of((chip ^ turn) * count, count), count), :]


def attend_first_kernel(*refs, chips, heads):
    mine, partner = refs[:chips], refs[chips : 2 * chips]
    outs, (q_all, k_all, v_all) = refs[2 * chips : 3 * chips], refs[3 * chips : 3 * chips + 3]
    o_all = refs[-1]
    length = mine[0].shape[0]
    wide_k = heads * KD
    chip, core = seat()
    ones = jnp.ones((length, VD), jnp.bfloat16)
    for turn in range(chips):
        there = chip ^ turn
        q_all[pl.ds(pl.multiple_of(there * length, length), length), :] = mine[turn][:, :wide_k]
        for ref, side in ((mine[turn], core), (partner[turn], 1 - core)):
            rows = pl.ds(pl.multiple_of((2 * there + side) * length, length), length)
            k_all[rows, :] = ref[:, wide_k : 2 * wide_k]
            for head in range(heads):
                at = 2 * wide_k + head * VD
                v_all[rows, 2 * head * VD : (2 * head + 1) * VD] = ref[:, at : at + VD]
                v_all[rows, (2 * head + 1) * VD : (2 * head + 2) * VD] = ones
    attend_rows(q_all, k_all, v_all, o_all, 0, core, chips, heads)
    deal(o_all, outs, chip)


def attend_later_kernel(q_all, k_all, v_all, *refs, chips, heads, rows_from):
    chip, core = seat()
    attend_rows(q_all, k_all, v_all, refs[-1], rows_from, core, chips, heads)
    deal(refs[-1], refs[:-1], chip)


def attend(mine, partner, heads, cuts):
    chips, (length, _), kind = len(mine), mine[0].shape, mine[0].dtype
    whole, sizes = 2 * chips * length, [high - low for low, high in zip(cuts, cuts[1:])]
    each = [pltpu.VMEM((size, heads * VD), kind) for size in sizes]
    *first, q_all, k_all, v_all = pl.pallas_call(
        functools.partial(attend_first_kernel, chips=chips, heads=heads),
        out_shape=(
            *(each[0],) * chips,
            pltpu.VMEM((whole // 2, heads * KD), kind),
            pltpu.VMEM((whole, heads * KD), kind),
            pltpu.VMEM((whole, 2 * heads * VD), kind),
        ),
        scratch_shapes=[pltpu.VMEM((chips * sizes[0], heads * VD), kind)],
        compiler_params=room(20),
        name="attend0",
    )(*in_vmem(*mine, *partner))
    results = [first]
    for part in range(1, len(sizes)):
        results.append(
            pl.pallas_call(
                functools.partial(attend_later_kernel, chips=chips, heads=heads, rows_from=cuts[part]),
                out_shape=(each[part],) * chips,
                scratch_shapes=[pltpu.VMEM((chips * sizes[part], heads * VD), kind)],
                compiler_params=room(16),
            )(*in_vmem(q_all, k_all, v_all))
        )
    return results


def block_at(slot):
    rank = lax.axis_index("head")
    turns = [(3, 3, 0, 0), (2, 2, 1, 1), (1, 0, 3, 2), (0, 1, 2, 3)][slot]
    block = jnp.int32(turns[0])
    for other in range(1, 4):
        block = jnp.where(rank == other, jnp.int32(turns[other]), block)
    return block


def project_kernel(*refs, chips, chunks, jobs):
    pieces, w_ref, outs = refs[: chunks * chips], refs[chunks * chips], refs[chunks * chips + 1 :]
    depth, columns = pieces[0].shape[1], outs[0].shape[1]
    here, _ = seat()
    for (slot, wanted), out in zip(jobs, outs):
        at = pl.ds(pl.multiple_of(block_at(slot) * columns, columns), columns)
        low = 0
        for chunk in wanted:
            total = None
            for turn in range(chips):
                rows = pl.ds(pl.multiple_of((here ^ turn) * depth, depth), depth)
                part = jnp.dot(
                    pieces[chunk * chips + turn][...], w_ref[rows, at], preferred_element_type=jnp.float32
                )
                total = part if total is None else total + part
            out[low : low + total.shape[0], :] = total.astype(out.dtype)
            low += total.shape[0]


def project(chunks, weight, columns, jobs, kinds):
    sizes = [pieces[0].shape[0] for pieces in chunks]
    return pl.pallas_call(
        functools.partial(project_kernel, chips=len(chunks[0]), chunks=len(chunks), jobs=jobs),
        out_shape=tuple(
            pltpu.VMEM((sum(sizes[chunk] for chunk in wanted), columns), kind)
            for (_, wanted), kind in zip(jobs, kinds)
        ),
        compiler_params=room(12),
    )(*in_vmem(*(piece for pieces in chunks for piece in pieces), weight))


def join_kernel(one, other, out, *, low):
    rows = one[low : low + other.shape[0], :].astype(jnp.float32)
    out[...] = (rows + other[...].astype(jnp.float32)).astype(out.dtype)


def join(one, other, low):
    return pl.pallas_call(
        functools.partial(join_kernel, low=low),
        out_shape=pltpu.VMEM(other.shape, other.dtype),
        compiler_params=room(4),
        name="join",
    )(*in_vmem(one, other))


def finish_kernel(own, third, *refs):
    lates, lasts, out = refs[: len(refs) // 2], refs[len(refs) // 2 : -1], refs[-1]
    low = 0
    for late, last in zip(lates, lasts):
        rows = slice(low, low + late.shape[0])
        total = own[rows, :] + third[rows, :].astype(jnp.float32)
        total = total + late[...].astype(jnp.float32) + last[...].astype(jnp.float32)
        out[rows, :] = total.astype(out.dtype)
        low += late.shape[0]


def finish(own, third, lates, lasts):
    return pl.pallas_call(
        finish_kernel,
        out_shape=jax.ShapeDtypeStruct(own.shape, third.dtype),
        compiler_params=room(8),
        name="finish",
    )(*in_vmem(own, third, *lates, *lasts))


def exchanged(queries, key_vectors, value_vectors, out_weight):
    seq, ranks = lax.axis_size("seq"), lax.axis_size("head")
    chips = seq // 2
    heads = out_weight.shape[0] // VD // chips
    columns = out_weight.shape[1] // ranks
    length = queries.shape[0]
    cuts = (0, length // 2, length)
    bf16, f32 = jnp.bfloat16, jnp.float32

    packed = pack(queries, key_vectors, value_vectors, chips)
    mine = [packed[0]] + [swap(packed[turn], "seq", 2 * turn) for turn in range(1, chips)]
    partner = [swap(piece, "seq", 1) for piece in mine]
    results = attend(mine, partner, heads, cuts)
    weight = stage(out_weight)
    chunks = [[outs[0]] + [swap(outs[turn], "seq", 2 * turn) for turn in range(1, chips)] for outs in results]

    def hop(value, source, target):
        pairs = [(source, target), (ranks - 1 - source, ranks - 1 - target)]
        return lax.ppermute(value, "head", pairs)

    parts = range(len(chunks))
    to_first, to_second = [None, None], [None, None]
    (to_first[0],) = project(chunks[:1], weight, columns, ((0, (0,)),), (bf16,))
    (to_second[0],) = project(chunks[:1], weight, columns, ((1, (0,)),), (bf16,))
    (to_first[1],) = project(chunks[1:], weight, columns, ((0, (0,)),), (bf16,))
    to_second[1], to_third, own = project(
        chunks, weight, columns, ((1, (1,)), (2, (0, 1)), (3, (0, 1))), (bf16, bf16, f32)
    )
    first = [hop(to_first[part], 0, 1) for part in parts]
    second = [hop(to_second[part], 0, 1) for part in parts]
    third = hop(to_third, 0, 1)
    middle = [hop(join(to_first[part], first[part], 0), 1, 2) for part in parts]
    late = [hop(join(to_second[part], second[part], 0), 1, 2) for part in parts]
    last = [hop(join(to_third, middle[part], cuts[part]), 2, 3) for part in parts]
    return finish(own, third, late, last)


def gathered(queries, key_vectors, value_vectors, out_weight):
    heads_here = out_weight.shape[0] // VD
    length = queries.shape[0]
    here = lax.axis_index("seq")
    k_all = lax.all_gather(key_vectors, "seq", axis=0, tiled=True)
    v_all = lax.all_gather(value_vectors, "seq", axis=0, tiled=True)
    rows = here * length + jnp.arange(length, dtype=jnp.int32)
    causal = jnp.arange(k_all.shape[0], dtype=jnp.int32)[None, :] <= rows[:, None]
    results = []
    for head in range(heads_here):
        q = queries[:, head * KD : (head + 1) * KD]
        k = k_all[:, head * KD : (head + 1) * KD]
        v = v_all[:, head * VD : (head + 1) * VD]
        scores = jnp.einsum("bd,td->bt", q, k, preferred_element_type=jnp.float32) * KD ** (-0.5)
        weights = jnp.where(causal, 1.0 + scores + 0.5 * scores * scores, 0.0).astype(jnp.bfloat16)
        numer = jnp.dot(weights, v, preferred_element_type=jnp.float32)
        denom = jnp.sum(weights, axis=-1, dtype=jnp.float32)
        results.append((numer / denom[:, None]).astype(jnp.bfloat16))
    attention = jnp.concatenate(results, axis=1)
    partial = jnp.dot(attention, out_weight, preferred_element_type=jnp.float32)
    mixed = lax.psum_scatter(partial, "head", scatter_dimension=1, tiled=True)
    return mixed.astype(jnp.bfloat16)


def planned(seq, ranks, heads_here):
    chips = seq // 2
    paired = seq == 2 * chips and chips > 0 and chips & (chips - 1) == 0
    return paired and ranks == 4 and heads_here % chips == 0 and (heads_here // chips * KD) % 128 == 0


def per_device(queries, key_vectors, value_vectors, out_weight):
    if planned(lax.axis_size("seq"), lax.axis_size("head"), out_weight.shape[0] // VD):
        return exchanged(queries, key_vectors, value_vectors, out_weight)
    return gathered(queries, key_vectors, value_vectors, out_weight)


def solution(mesh):
    placed = (P("seq", "head"), P("seq", "head"), P("seq", "head"), P("head", None))
    step = jax.shard_map(
        per_device, mesh=mesh, in_specs=placed, out_specs=P("seq", "head"), check_vma=False
    )
    seq, ranks = mesh.shape["seq"], mesh.shape["head"]

    def whole(queries, key_vectors, value_vectors, out_weight):
        run = step
        if planned(seq, ranks, out_weight.shape[0] // ranks // VD):
            run = step
        return run(queries, key_vectors, value_vectors, out_weight)

    return whole
```

```python
import functools

import jax
import jax.numpy as jnp
from jax import lax
from jax.experimental import pallas as pl
from jax.experimental.pallas import tpu as pltpu
from jax.sharding import PartitionSpec as P


KD = 64
VD = 128


def swap(value, axis, bits):
    count = lax.axis_size(axis)
    return lax.ppermute(value, axis, [(i, i ^ bits) for i in range(count)])


def in_vmem(*values):
    return [pltpu.with_memory_space_constraint(value, pltpu.VMEM) for value in values]


def in_hbm(*values):
    return [pltpu.with_memory_space_constraint(value, pltpu.HBM) for value in values]


def room(mebibytes):
    return pltpu.CompilerParams(vmem_limit_bytes=mebibytes << 20)


def seat():
    here = lax.axis_index("seq")
    return here >> 1, here & 1


def stacks(count, tiles):
    high = -(-count // (16 * tiles)) * 16
    return high, [(at, min(high, count - at)) for at in range(0, count, high)]


def pack_kernel(q_ref, k_ref, v_ref, *refs, first):
    half = (len(refs) - 1) // 2
    outs, laters, arrived = refs[:half], refs[half:-1], refs[-1]
    length, wide_k = q_ref.shape[0], laters[0].shape[1]
    _, rows_of = stacks(first, outs[0].shape[1] // wide_k)
    here, _ = seat()
    copies = []

    def copy(source, target):
        copies.append(pltpu.make_async_copy(source, target, arrived.at[len(copies)]))
        copies[-1].start()

    for turn in (*range(1, half), 0):
        out, later = outs[turn], laters[turn]
        narrow = pl.ds(pl.multiple_of((here ^ turn) * wide_k, wide_k), wide_k)
        wide = pl.ds(pl.multiple_of((here ^ turn) * 2 * wide_k, 2 * wide_k), 2 * wide_k)
        copy(k_ref.at[:, narrow], out.at[:length, :wide_k])
        copy(v_ref.at[:, wide], out.at[:length, wide_k:])
        for tile, (at, size) in enumerate(rows_of):
            copy(
                q_ref.at[at : at + size, narrow],
                out.at[length : length + size, tile * wide_k : (tile + 1) * wide_k],
            )
        copy(q_ref.at[first:, narrow], later)
    for each in copies:
        each.wait()


def pack(queries, keys, values, chips, first):
    (length, width), kind = queries.shape, queries.dtype
    wide_k = width // chips
    high, rows_of = stacks(first, 3)
    return pl.pallas_call(
        functools.partial(pack_kernel, first=first),
        out_shape=(
            *(pltpu.VMEM((length + high, 3 * wide_k), kind),) * chips,
            *(pltpu.VMEM((length - first, wide_k), kind),) * chips,
        ),
        in_specs=[pl.BlockSpec(memory_space=pltpu.HBM)] * 3,
        scratch_shapes=[pltpu.SemaphoreType.DMA(((3 + len(rows_of)) * chips,))],
        compiler_params=room(8),
        name="pack",
    )(*in_hbm(queries, keys, values))


def stage_kernel(w_ref, out, arrived):
    copy = pltpu.make_async_copy(w_ref, out, arrived.at[0])
    copy.start()
    copy.wait()


def stage(weight):
    return pl.pallas_call(
        stage_kernel,
        out_shape=pltpu.VMEM(weight.shape, weight.dtype),
        in_specs=[pl.BlockSpec(memory_space=pltpu.HBM)],
        scratch_shapes=[pltpu.SemaphoreType.DMA((1,))],
        compiler_params=room(4),
        name="stage",
    )(*in_hbm(weight))


def attend_rows(q_part, k_all, v_all, o_all, rows_from, core, chips, heads):
    length, wide_k = k_all.shape[0] // (2 * chips), heads * KD
    count = o_all.shape[0] // chips
    row = lax.broadcasted_iota(jnp.int32, (count, 2 * length), 0) + (core * length + rows_from)
    seen = lax.broadcasted_iota(jnp.int32, (count, 2 * length), 1) <= row
    lane = lax.broadcasted_iota(jnp.int32, (count, wide_k), 1) // KD
    for index in range(chips):
        q = q_part[index * count : (index + 1) * count, :] * jnp.bfloat16(KD ** (-0.5))
        for head in range(heads):
            own = jnp.where(lane == head, q, jnp.bfloat16(0))
            columns = slice(2 * head * VD, (2 * head + 2) * VD)
            total = None
            for block in range(index + 1):
                rows = slice(2 * block * length, 2 * (block + 1) * length)
                scores = lax.dot_general(
                    own, k_all[rows, :], (((1,), (1,)), ((), ())), preferred_element_type=jnp.float32
                )
                raised = scores + 1.0
                weights = raised * raised + 1.0
                if block == index:
                    weights = jnp.where(seen, weights, 0.0)
                part = jnp.dot(
                    weights.astype(jnp.bfloat16), v_all[rows, columns], preferred_element_type=jnp.float32
                )
                total = part if total is None else total + part
            o_all[index * count : (index + 1) * count, head * VD : (head + 1) * VD] = (
                total[:, :VD] / total[:, VD:]
            ).astype(jnp.bfloat16)


def deal(o_all, outs, chip):
    count = outs[0].shape[0]
    for turn, out in enumerate(outs):
        out[...] = o_all[pl.ds(pl.multiple_of((chip ^ turn) * count, count), count), :]


def attend_first_kernel(*refs, chips, heads):
    mine, partner = refs[:chips], refs[chips : 2 * chips]
    outs, (k_all, v_all) = refs[2 * chips : 3 * chips], refs[3 * chips : 3 * chips + 2]
    q_part, o_all = refs[-2:]
    wide_k = heads * KD
    length, count = k_all.shape[0] // (2 * chips), q_part.shape[0] // chips
    _, rows_of = stacks(count, mine[0].shape[1] // wide_k)
    chip, core = seat()
    ones = jnp.ones((length, VD), jnp.bfloat16)
    for turn in range(chips):
        there = chip ^ turn
        for tile, (at, size) in enumerate(rows_of):
            q_part[pl.ds(pl.multiple_of(there * count + at, 16), size), :] = mine[turn][
                length : length + size, tile * wide_k : (tile + 1) * wide_k
            ]
        for ref, side in ((mine[turn], core), (partner[turn], 1 - core)):
            rows = pl.ds(pl.multiple_of((2 * there + side) * length, length), length)
            k_all[rows, :] = ref[:length, :wide_k]
            for head in range(heads):
                at = wide_k + head * VD
                v_all[rows, 2 * head * VD : (2 * head + 1) * VD] = ref[:length, at : at + VD]
                v_all[rows, (2 * head + 1) * VD : (2 * head + 2) * VD] = ones
    attend_rows(q_part, k_all, v_all, o_all, 0, core, chips, heads)
    deal(o_all, outs, chip)


def attend_later_kernel(k_all, v_all, *refs, chips, heads, rows_from):
    queries, outs, (q_part, o_all) = refs[:chips], refs[chips : 2 * chips], refs[2 * chips :]
    count = q_part.shape[0] // chips
    chip, core = seat()
    for turn in range(chips):
        q_part[pl.ds(pl.multiple_of((chip ^ turn) * count, count), count), :] = queries[turn][...]
    attend_rows(q_part, k_all, v_all, o_all, rows_from, core, chips, heads)
    deal(o_all, outs, chip)


def attend(mine, partner, later, heads, cuts):
    chips, length, kind = len(mine), cuts[-1], mine[0].dtype
    whole, (first, second) = 2 * chips * length, (cuts[1], cuts[2] - cuts[1])

    def scratch(size):
        return [pltpu.VMEM((chips * size, heads * KD), kind), pltpu.VMEM((chips * size, heads * VD), kind)]

    *one, k_all, v_all = pl.pallas_call(
        functools.partial(attend_first_kernel, chips=chips, heads=heads),
        out_shape=(
            *(pltpu.VMEM((first, heads * VD), kind),) * chips,
            pltpu.VMEM((whole, heads * KD), kind),
            pltpu.VMEM((whole, 2 * heads * VD), kind),
        ),
        scratch_shapes=scratch(first),
        compiler_params=room(20),
        name="attend0",
    )(*in_vmem(*mine, *partner))
    other = pl.pallas_call(
        functools.partial(attend_later_kernel, chips=chips, heads=heads, rows_from=first),
        out_shape=(pltpu.VMEM((second, heads * VD), kind),) * chips,
        scratch_shapes=scratch(second),
        compiler_params=room(16),
        name="attend1",
    )(*in_vmem(k_all, v_all, *later))
    return [one, other]


def block_at(slot):
    rank = lax.axis_index("head")
    turns = [(3, 3, 0, 0), (2, 2, 1, 1), (1, 0, 3, 2), (0, 1, 2, 3)][slot]
    block = jnp.int32(turns[0])
    for other in range(1, 4):
        block = jnp.where(rank == other, jnp.int32(turns[other]), block)
    return block


def project_kernel(*refs, chips, chunks, jobs):
    pieces, w_ref, outs = refs[: chunks * chips], refs[chunks * chips], refs[chunks * chips + 1 :]
    depth, columns = pieces[0].shape[1], outs[0].shape[1]
    here, _ = seat()
    for (slot, wanted), out in zip(jobs, outs):
        at = pl.ds(pl.multiple_of(block_at(slot) * columns, columns), columns)
        low = 0
        for chunk in wanted:
            total = None
            for turn in range(chips):
                rows = pl.ds(pl.multiple_of((here ^ turn) * depth, depth), depth)
                part = jnp.dot(
                    pieces[chunk * chips + turn][...], w_ref[rows, at], preferred_element_type=jnp.float32
                )
                total = part if total is None else total + part
            out[low : low + total.shape[0], :] = total.astype(out.dtype)
            low += total.shape[0]


def project(chunks, weight, columns, jobs, kinds):
    sizes = [pieces[0].shape[0] for pieces in chunks]
    return pl.pallas_call(
        functools.partial(project_kernel, chips=len(chunks[0]), chunks=len(chunks), jobs=jobs),
        out_shape=tuple(
            pltpu.VMEM((sum(sizes[chunk] for chunk in wanted), columns), kind)
            for (_, wanted), kind in zip(jobs, kinds)
        ),
        compiler_params=room(12),
    )(*in_vmem(*(piece for pieces in chunks for piece in pieces), weight))


def join_kernel(one, other, out, *, low):
    rows = one[low : low + other.shape[0], :].astype(jnp.float32)
    out[...] = (rows + other[...].astype(jnp.float32)).astype(out.dtype)


def join(one, other, low):
    return pl.pallas_call(
        functools.partial(join_kernel, low=low),
        out_shape=pltpu.VMEM(other.shape, other.dtype),
        compiler_params=room(4),
        name="join",
    )(*in_vmem(one, other))


def finish_kernel(own, third, *refs, cuts, arrivals):
    out, rows, sent = refs[-3:]
    copies, at = [], 0
    for low, high, count in zip(cuts, cuts[1:], arrivals):
        total = own[low:high, :] + third[low:high, :].astype(jnp.float32)
        for part in refs[at : at + count]:
            total = total + part[...].astype(jnp.float32)
        at += count
        rows[low:high, :] = total.astype(rows.dtype)
        copies.append(
            pltpu.make_async_copy(rows.at[low:high, :], out.at[low:high, :], sent.at[len(copies)])
        )
        copies[-1].start()
    for copy in copies:
        copy.wait()


def finish(own, third, parts, cuts):
    flat = [part for some in parts for part in some]
    return pl.pallas_call(
        functools.partial(finish_kernel, cuts=cuts, arrivals=tuple(len(some) for some in parts)),
        out_shape=jax.ShapeDtypeStruct(own.shape, third.dtype),
        in_specs=[pl.BlockSpec(memory_space=pltpu.VMEM)] * (2 + len(flat)),
        out_specs=pl.BlockSpec(memory_space=pltpu.HBM),
        scratch_shapes=[pltpu.VMEM(own.shape, third.dtype), pltpu.SemaphoreType.DMA((len(parts),))],
        compiler_params=room(8),
        name="finish",
    )(*in_vmem(own, third, *flat))


def exchanged(queries, key_vectors, value_vectors, out_weight):
    seq, ranks = lax.axis_size("seq"), lax.axis_size("head")
    chips = seq // 2
    heads = out_weight.shape[0] // VD // chips
    columns = out_weight.shape[1] // ranks
    length = queries.shape[0]
    cuts = (0, length // 2, length)
    bf16, f32 = jnp.bfloat16, jnp.float32

    packed = pack(queries, key_vectors, value_vectors, chips, cuts[1])
    packed, later = packed[:chips], packed[chips:]
    mine = [packed[0]] + [swap(packed[turn], "seq", 2 * turn) for turn in range(1, chips)]
    partner = [swap(piece, "seq", 1) for piece in mine]
    later = [later[0]] + [swap(later[turn], "seq", 2 * turn) for turn in range(1, chips)]
    results = attend(mine, partner, later, heads, cuts)
    weight = stage(out_weight)
    chunks = [[outs[0]] + [swap(outs[turn], "seq", 2 * turn) for turn in range(1, chips)] for outs in results]

    def hop(value, source, target):
        pairs = [(source, target), (ranks - 1 - source, ranks - 1 - target)]
        return lax.ppermute(value, "head", pairs)

    to_first, to_second = [None, None], [None, None]
    (to_first[0],) = project(chunks[:1], weight, columns, ((0, (0,)),), (bf16,))
    (to_second[0],) = project(chunks[:1], weight, columns, ((1, (0,)),), (bf16,))
    (to_first[1],) = project(chunks[1:], weight, columns, ((0, (0,)),), (bf16,))
    beside, to_second[1], to_third, own = project(
        chunks, weight, columns, ((2, (1,)), (1, (1,)), (2, (0, 1)), (3, (0, 1))), (bf16, bf16, bf16, f32)
    )
    first = [hop(value, 0, 1) for value in to_first]
    second = [hop(value, 0, 1) for value in to_second]
    third = hop(to_third, 0, 1)
    joined = [join(mine, other, 0) for mine, other in zip(to_first, first)]
    late = [hop(join(mine, other, 0), 1, 2) for mine, other in zip(to_second, second)]
    last = hop(join(to_third, hop(joined[0], 1, 2), 0), 2, 3)
    straight, beside = hop(joined[1], 1, 3), hop(beside, 2, 3)
    return finish(own, third, ((late[0], last), (late[1], beside, straight)), cuts)


def gathered(queries, key_vectors, value_vectors, out_weight):
    heads_here = out_weight.shape[0] // VD
    length = queries.shape[0]
    here = lax.axis_index("seq")
    k_all = lax.all_gather(key_vectors, "seq", axis=0, tiled=True)
    v_all = lax.all_gather(value_vectors, "seq", axis=0, tiled=True)
    rows = here * length + jnp.arange(length, dtype=jnp.int32)
    causal = jnp.arange(k_all.shape[0], dtype=jnp.int32)[None, :] <= rows[:, None]
    results = []
    for head in range(heads_here):
        q = queries[:, head * KD : (head + 1) * KD]
        k = k_all[:, head * KD : (head + 1) * KD]
        v = v_all[:, head * VD : (head + 1) * VD]
        scores = jnp.einsum("bd,td->bt", q, k, preferred_element_type=jnp.float32) * KD ** (-0.5)
        weights = jnp.where(causal, 1.0 + scores + 0.5 * scores * scores, 0.0).astype(jnp.bfloat16)
        numer = jnp.dot(weights, v, preferred_element_type=jnp.float32)
        denom = jnp.sum(weights, axis=-1, dtype=jnp.float32)
        results.append((numer / denom[:, None]).astype(jnp.bfloat16))
    attention = jnp.concatenate(results, axis=1)
    partial = jnp.dot(attention, out_weight, preferred_element_type=jnp.float32)
    mixed = lax.psum_scatter(partial, "head", scatter_dimension=1, tiled=True)
    return mixed.astype(jnp.bfloat16)


def planned(seq, ranks, heads_here):
    chips = seq // 2
    paired = seq == 2 * chips and chips > 0 and chips & (chips - 1) == 0
    return paired and ranks == 4 and heads_here % chips == 0 and (heads_here // chips * KD) % 128 == 0


def per_device(queries, key_vectors, value_vectors, out_weight):
    if planned(lax.axis_size("seq"), lax.axis_size("head"), out_weight.shape[0] // VD):
        return exchanged(queries, key_vectors, value_vectors, out_weight)
    return gathered(queries, key_vectors, value_vectors, out_weight)


def solution(mesh):
    placed = (P("seq", "head"), P("seq", "head"), P("seq", "head"), P("head", None))
    step = jax.shard_map(
        per_device, mesh=mesh, in_specs=placed, out_specs=P("seq", "head"), check_vma=False
    )
    seq, ranks = mesh.shape["seq"], mesh.shape["head"]

    def whole(queries, key_vectors, value_vectors, out_weight):
        run = step
        if planned(seq, ranks, out_weight.shape[0] // ranks // VD):
            run = step
        return run(queries, key_vectors, value_vectors, out_weight)

    return whole
```

```python
import functools

import jax
import jax.numpy as jnp
from jax import lax
from jax.experimental import pallas as pl
from jax.experimental.pallas import tpu as pltpu
from jax.sharding import PartitionSpec as P


KD = 64
VD = 128


def swap(value, axis, bits):
    count = lax.axis_size(axis)
    return lax.ppermute(value, axis, [(i, i ^ bits) for i in range(count)])


def in_vmem(*values):
    return [pltpu.with_memory_space_constraint(value, pltpu.VMEM) for value in values]


def in_hbm(*values):
    return [pltpu.with_memory_space_constraint(value, pltpu.HBM) for value in values]


def room(mebibytes):
    return pltpu.CompilerParams(vmem_limit_bytes=mebibytes << 20)


def seat():
    here = lax.axis_index("seq")
    return here >> 1, here & 1


def stacks(count, tiles):
    high = -(-count // (16 * tiles)) * 16
    return high, [(at, min(high, count - at)) for at in range(0, count, high)]


def pack_kernel(q_ref, k_ref, v_ref, *refs, first):
    half = (len(refs) - 1) // 2
    outs, laters, arrived = refs[:half], refs[half:-1], refs[-1]
    length, wide_k = q_ref.shape[0], laters[0].shape[1]
    _, rows_of = stacks(first, outs[0].shape[1] // wide_k)
    here, _ = seat()
    copies = []

    def copy(source, target):
        copies.append(pltpu.make_async_copy(source, target, arrived.at[len(copies)]))
        copies[-1].start()

    for turn in (*range(1, half), 0):
        out, later = outs[turn], laters[turn]
        narrow = pl.ds(pl.multiple_of((here ^ turn) * wide_k, wide_k), wide_k)
        wide = pl.ds(pl.multiple_of((here ^ turn) * 2 * wide_k, 2 * wide_k), 2 * wide_k)
        copy(k_ref.at[:, narrow], out.at[:length, :wide_k])
        copy(v_ref.at[:, wide], out.at[:length, wide_k:])
        for tile, (at, size) in enumerate(rows_of):
            copy(
                q_ref.at[at : at + size, narrow],
                out.at[length : length + size, tile * wide_k : (tile + 1) * wide_k],
            )
        copy(q_ref.at[first:, narrow], later)
    for each in copies:
        each.wait()


def pack(queries, keys, values, chips, first):
    (length, width), kind = queries.shape, queries.dtype
    wide_k = width // chips
    high, rows_of = stacks(first, 3)
    return pl.pallas_call(
        functools.partial(pack_kernel, first=first),
        out_shape=(
            *(pltpu.VMEM((length + high, 3 * wide_k), kind),) * chips,
            *(pltpu.VMEM((length - first, wide_k), kind),) * chips,
        ),
        in_specs=[pl.BlockSpec(memory_space=pltpu.HBM)] * 3,
        scratch_shapes=[pltpu.SemaphoreType.DMA(((3 + len(rows_of)) * chips,))],
        compiler_params=room(8),
        name="pack",
    )(*in_hbm(queries, keys, values))


def stage_kernel(w_ref, out, arrived):
    copy = pltpu.make_async_copy(w_ref, out, arrived.at[0])
    copy.start()
    copy.wait()


def stage(weight):
    return pl.pallas_call(
        stage_kernel,
        out_shape=pltpu.VMEM(weight.shape, weight.dtype),
        in_specs=[pl.BlockSpec(memory_space=pltpu.HBM)],
        scratch_shapes=[pltpu.SemaphoreType.DMA((1,))],
        compiler_params=room(4),
        name="stage",
    )(*in_hbm(weight))


def attend_rows(q_part, k_all, v_all, o_all, rows_from, core, chips, heads):
    length, wide_k = k_all.shape[0] // (2 * chips), heads * KD
    count = o_all.shape[0] // chips
    reach = length + rows_from + count
    row = lax.broadcasted_iota(jnp.int32, (count, reach), 0) + (core * length + rows_from)
    seen = lax.broadcasted_iota(jnp.int32, (count, reach), 1) <= row
    seen = jnp.concatenate([seen] * heads, axis=0)
    lane = lax.broadcasted_iota(jnp.int32, (count, wide_k), 1) // KD
    for index in range(chips):
        q = q_part[index * count : (index + 1) * count, :] * jnp.bfloat16(KD ** (-0.5))
        stacked = jnp.concatenate([jnp.where(lane == head, q, jnp.bfloat16(0)) for head in range(heads)], axis=0)
        total = denominator = None
        for block in range(index + 1):
            at = 2 * block * length
            rows = slice(at, at + (reach if block == index else 2 * length))
            scores = lax.dot_general(
                stacked, k_all[rows, :], (((1,), (1,)), ((), ())), preferred_element_type=jnp.float32
            )
            raised = scores + 1.0
            weights = raised * raised + 1.0
            if block == index:
                weights = jnp.where(seen, weights, 0.0)
            weights = weights.astype(jnp.bfloat16)
            part = jnp.dot(weights, v_all[rows, :], preferred_element_type=jnp.float32)
            total = part if total is None else total + part
            sums = jnp.sum(weights.astype(jnp.float32), axis=1, keepdims=True)
            denominator = sums if denominator is None else denominator + sums
        for head in range(heads):
            own = slice(head * count, (head + 1) * count)
            lanes = slice(head * VD, (head + 1) * VD)
            o_all[index * count : (index + 1) * count, lanes] = (total[own, lanes] / denominator[own]).astype(
                jnp.bfloat16
            )


def deal(o_all, outs, chip):
    count = outs[0].shape[0]
    for turn, out in enumerate(outs):
        out[...] = o_all[pl.ds(pl.multiple_of((chip ^ turn) * count, count), count), :]


def attend_first_kernel(*refs, chips, heads):
    mine, partner = refs[:chips], refs[chips : 2 * chips]
    outs, (k_all, v_all) = refs[2 * chips : 3 * chips], refs[3 * chips : 3 * chips + 2]
    q_part, o_all = refs[-2:]
    wide_k = heads * KD
    length, count = k_all.shape[0] // (2 * chips), q_part.shape[0] // chips
    _, rows_of = stacks(count, mine[0].shape[1] // wide_k)
    chip, core = seat()
    for turn in range(chips):
        there = chip ^ turn
        for tile, (at, size) in enumerate(rows_of):
            q_part[pl.ds(pl.multiple_of(there * count + at, 16), size), :] = mine[turn][
                length : length + size, tile * wide_k : (tile + 1) * wide_k
            ]
        for ref, side in ((mine[turn], core), (partner[turn], 1 - core)):
            rows = pl.ds(pl.multiple_of((2 * there + side) * length, length), length)
            k_all[rows, :] = ref[:length, :wide_k]
            v_all[rows, :] = ref[:length, wide_k:]
    attend_rows(q_part, k_all, v_all, o_all, 0, core, chips, heads)
    deal(o_all, outs, chip)


def attend_later_kernel(k_all, v_all, *refs, chips, heads, rows_from):
    queries, outs, (q_part, o_all) = refs[:chips], refs[chips : 2 * chips], refs[2 * chips :]
    count = q_part.shape[0] // chips
    chip, core = seat()
    for turn in range(chips):
        q_part[pl.ds(pl.multiple_of((chip ^ turn) * count, count), count), :] = queries[turn][...]
    attend_rows(q_part, k_all, v_all, o_all, rows_from, core, chips, heads)
    deal(o_all, outs, chip)


def attend(mine, partner, later, heads, cuts):
    chips, length, kind = len(mine), cuts[-1], mine[0].dtype
    whole, (first, second) = 2 * chips * length, (cuts[1], cuts[2] - cuts[1])

    def scratch(size):
        return [pltpu.VMEM((chips * size, heads * KD), kind), pltpu.VMEM((chips * size, heads * VD), kind)]

    *one, k_all, v_all = pl.pallas_call(
        functools.partial(attend_first_kernel, chips=chips, heads=heads),
        out_shape=(
            *(pltpu.VMEM((first, heads * VD), kind),) * chips,
            pltpu.VMEM((whole, heads * KD), kind),
            pltpu.VMEM((whole, heads * VD), kind),
        ),
        scratch_shapes=scratch(first),
        compiler_params=room(20),
        name="attend0",
    )(*in_vmem(*mine, *partner))
    other = pl.pallas_call(
        functools.partial(attend_later_kernel, chips=chips, heads=heads, rows_from=first),
        out_shape=(pltpu.VMEM((second, heads * VD), kind),) * chips,
        scratch_shapes=scratch(second),
        compiler_params=room(16),
        name="attend1",
    )(*in_vmem(k_all, v_all, *later))
    return [one, other]


def block_at(slot):
    rank = lax.axis_index("head")
    turns = [(3, 3, 0, 0), (2, 2, 1, 1), (1, 0, 3, 2), (0, 1, 2, 3)][slot]
    block = jnp.int32(turns[0])
    for other in range(1, 4):
        block = jnp.where(rank == other, jnp.int32(turns[other]), block)
    return block


def project_kernel(*refs, chips, chunks, jobs):
    pieces, w_ref, outs = refs[: chunks * chips], refs[chunks * chips], refs[chunks * chips + 1 :]
    depth, columns = pieces[0].shape[1], outs[0].shape[1]
    here, _ = seat()
    for (slot, wanted), out in zip(jobs, outs):
        at = pl.ds(pl.multiple_of(block_at(slot) * columns, columns), columns)
        low = 0
        for chunk in wanted:
            total = None
            for turn in range(chips):
                rows = pl.ds(pl.multiple_of((here ^ turn) * depth, depth), depth)
                part = jnp.dot(
                    pieces[chunk * chips + turn][...], w_ref[rows, at], preferred_element_type=jnp.float32
                )
                total = part if total is None else total + part
            out[low : low + total.shape[0], :] = total.astype(out.dtype)
            low += total.shape[0]


def project(chunks, weight, columns, jobs, kinds):
    sizes = [pieces[0].shape[0] for pieces in chunks]
    return pl.pallas_call(
        functools.partial(project_kernel, chips=len(chunks[0]), chunks=len(chunks), jobs=jobs),
        out_shape=tuple(
            pltpu.VMEM((sum(sizes[chunk] for chunk in wanted), columns), kind)
            for (_, wanted), kind in zip(jobs, kinds)
        ),
        compiler_params=room(12),
    )(*in_vmem(*(piece for pieces in chunks for piece in pieces), weight))


def join_kernel(one, other, out, *, low):
    rows = one[low : low + other.shape[0], :].astype(jnp.float32)
    out[...] = (rows + other[...].astype(jnp.float32)).astype(out.dtype)


def join(one, other, low):
    return pl.pallas_call(
        functools.partial(join_kernel, low=low),
        out_shape=pltpu.VMEM(other.shape, other.dtype),
        compiler_params=room(4),
        name="join",
    )(*in_vmem(one, other))


def finish_kernel(own, third, *refs, cuts, arrivals):
    out, rows, sent = refs[-3:]
    copies, at = [], 0
    for low, high, count in zip(cuts, cuts[1:], arrivals):
        total = own[low:high, :] + third[low:high, :].astype(jnp.float32)
        for part in refs[at : at + count]:
            total = total + part[...].astype(jnp.float32)
        at += count
        rows[low:high, :] = total.astype(rows.dtype)
        copies.append(
            pltpu.make_async_copy(rows.at[low:high, :], out.at[low:high, :], sent.at[len(copies)])
        )
        copies[-1].start()
    for copy in copies:
        copy.wait()


def finish(own, third, parts, cuts):
    flat = [part for some in parts for part in some]
    return pl.pallas_call(
        functools.partial(finish_kernel, cuts=cuts, arrivals=tuple(len(some) for some in parts)),
        out_shape=jax.ShapeDtypeStruct(own.shape, third.dtype),
        in_specs=[pl.BlockSpec(memory_space=pltpu.VMEM)] * (2 + len(flat)),
        out_specs=pl.BlockSpec(memory_space=pltpu.HBM),
        scratch_shapes=[pltpu.VMEM(own.shape, third.dtype), pltpu.SemaphoreType.DMA((len(parts),))],
        compiler_params=room(8),
        name="finish",
    )(*in_vmem(own, third, *flat))


def exchanged(queries, key_vectors, value_vectors, out_weight):
    seq, ranks = lax.axis_size("seq"), lax.axis_size("head")
    chips = seq // 2
    heads = out_weight.shape[0] // VD // chips
    columns = out_weight.shape[1] // ranks
    length = queries.shape[0]
    cuts = (0, length // 2, length)
    bf16, f32 = jnp.bfloat16, jnp.float32

    packed = pack(queries, key_vectors, value_vectors, chips, cuts[1])
    packed, later = packed[:chips], packed[chips:]
    mine = [packed[0]] + [swap(packed[turn], "seq", 2 * turn) for turn in range(1, chips)]
    partner = [swap(piece, "seq", 1) for piece in mine]
    later = [later[0]] + [swap(later[turn], "seq", 2 * turn) for turn in range(1, chips)]
    results = attend(mine, partner, later, heads, cuts)
    weight = stage(out_weight)
    chunks = [[outs[0]] + [swap(outs[turn], "seq", 2 * turn) for turn in range(1, chips)] for outs in results]

    def hop(value, source, target):
        pairs = [(source, target), (ranks - 1 - source, ranks - 1 - target)]
        return lax.ppermute(value, "head", pairs)

    to_first, to_second = [None, None], [None, None]
    (to_first[0],) = project(chunks[:1], weight, columns, ((0, (0,)),), (bf16,))
    (to_second[0],) = project(chunks[:1], weight, columns, ((1, (0,)),), (bf16,))
    (to_first[1],) = project(chunks[1:], weight, columns, ((0, (0,)),), (bf16,))
    beside, to_second[1], to_third, own = project(
        chunks, weight, columns, ((2, (1,)), (1, (1,)), (2, (0, 1)), (3, (0, 1))), (bf16, bf16, bf16, f32)
    )
    first = [hop(value, 0, 1) for value in to_first]
    second = [hop(value, 0, 1) for value in to_second]
    third = hop(to_third, 0, 1)
    joined = [join(mine, other, 0) for mine, other in zip(to_first, first)]
    late = [hop(join(mine, other, 0), 1, 2) for mine, other in zip(to_second, second)]
    last = hop(join(to_third, hop(joined[0], 1, 2), 0), 2, 3)
    straight, beside = hop(joined[1], 1, 3), hop(beside, 2, 3)
    return finish(own, third, ((late[0], last), (late[1], beside, straight)), cuts)


def gathered(queries, key_vectors, value_vectors, out_weight):
    heads_here = out_weight.shape[0] // VD
    length = queries.shape[0]
    here = lax.axis_index("seq")
    k_all = lax.all_gather(key_vectors, "seq", axis=0, tiled=True)
    v_all = lax.all_gather(value_vectors, "seq", axis=0, tiled=True)
    rows = here * length + jnp.arange(length, dtype=jnp.int32)
    causal = jnp.arange(k_all.shape[0], dtype=jnp.int32)[None, :] <= rows[:, None]
    results = []
    for head in range(heads_here):
        q = queries[:, head * KD : (head + 1) * KD]
        k = k_all[:, head * KD : (head + 1) * KD]
        v = v_all[:, head * VD : (head + 1) * VD]
        scores = jnp.einsum("bd,td->bt", q, k, preferred_element_type=jnp.float32) * KD ** (-0.5)
        weights = jnp.where(causal, 1.0 + scores + 0.5 * scores * scores, 0.0).astype(jnp.bfloat16)
        numer = jnp.dot(weights, v, preferred_element_type=jnp.float32)
        denom = jnp.sum(weights, axis=-1, dtype=jnp.float32)
        results.append((numer / denom[:, None]).astype(jnp.bfloat16))
    attention = jnp.concatenate(results, axis=1)
    partial = jnp.dot(attention, out_weight, preferred_element_type=jnp.float32)
    mixed = lax.psum_scatter(partial, "head", scatter_dimension=1, tiled=True)
    return mixed.astype(jnp.bfloat16)


def planned(seq, ranks, heads_here):
    chips = seq // 2
    paired = seq == 2 * chips and chips > 0 and chips & (chips - 1) == 0
    return paired and ranks == 4 and heads_here % chips == 0 and (heads_here // chips * KD) % 128 == 0


def per_device(queries, key_vectors, value_vectors, out_weight):
    if planned(lax.axis_size("seq"), lax.axis_size("head"), out_weight.shape[0] // VD):
        return exchanged(queries, key_vectors, value_vectors, out_weight)
    return gathered(queries, key_vectors, value_vectors, out_weight)


def solution(mesh):
    placed = (P("seq", "head"), P("seq", "head"), P("seq", "head"), P("head", None))
    step = jax.shard_map(
        per_device, mesh=mesh, in_specs=placed, out_specs=P("seq", "head"), check_vma=False
    )
    seq, ranks = mesh.shape["seq"], mesh.shape["head"]

    def whole(queries, key_vectors, value_vectors, out_weight):
        run = step
        if planned(seq, ranks, out_weight.shape[0] // ranks // VD):
            run = step
        return run(queries, key_vectors, value_vectors, out_weight)

    return whole
```

```python
import functools

import jax
import jax.numpy as jnp
from jax import lax
from jax.experimental import pallas as pl
from jax.experimental.pallas import tpu as pltpu
from jax.sharding import PartitionSpec as P


KD = 64
VD = 128


def swap(value, axis, bits):
    count = lax.axis_size(axis)
    return lax.ppermute(value, axis, [(i, i ^ bits) for i in range(count)])


def in_vmem(*values):
    return [pltpu.with_memory_space_constraint(value, pltpu.VMEM) for value in values]


def in_hbm(*values):
    return [pltpu.with_memory_space_constraint(value, pltpu.HBM) for value in values]


def room(mebibytes):
    return pltpu.CompilerParams(vmem_limit_bytes=mebibytes << 20)


def seat():
    here = lax.axis_index("seq")
    return here >> 1, here & 1


def stacks(count, tiles):
    high = -(-count // (16 * tiles)) * 16
    return high, [(at, min(high, count - at)) for at in range(0, count, high)]


def pack_kernel(q_ref, k_ref, v_ref, *refs, first):
    half = (len(refs) - 1) // 2
    outs, laters, arrived = refs[:half], refs[half:-1], refs[-1]
    length, wide_k = q_ref.shape[0], laters[0].shape[1]
    _, rows_of = stacks(first, outs[0].shape[1] // wide_k)
    here, _ = seat()
    copies = []

    def copy(source, target):
        copies.append(pltpu.make_async_copy(source, target, arrived.at[len(copies)]))
        copies[-1].start()

    for turn in (*range(1, half), 0):
        out, later = outs[turn], laters[turn]
        narrow = pl.ds(pl.multiple_of((here ^ turn) * wide_k, wide_k), wide_k)
        wide = pl.ds(pl.multiple_of((here ^ turn) * 2 * wide_k, 2 * wide_k), 2 * wide_k)
        copy(k_ref.at[:, narrow], out.at[:length, :wide_k])
        copy(v_ref.at[:, wide], out.at[:length, wide_k:])
        for tile, (at, size) in enumerate(rows_of):
            copy(
                q_ref.at[at : at + size, narrow],
                out.at[length : length + size, tile * wide_k : (tile + 1) * wide_k],
            )
        copy(q_ref.at[first:, narrow], later)
    for each in copies:
        each.wait()


def pack(queries, keys, values, chips, first):
    (length, width), kind = queries.shape, queries.dtype
    wide_k = width // chips
    high, rows_of = stacks(first, 3)
    return pl.pallas_call(
        functools.partial(pack_kernel, first=first),
        out_shape=(
            *(pltpu.VMEM((length + high, 3 * wide_k), kind),) * chips,
            *(pltpu.VMEM((length - first, wide_k), kind),) * chips,
        ),
        in_specs=[pl.BlockSpec(memory_space=pltpu.HBM)] * 3,
        scratch_shapes=[pltpu.SemaphoreType.DMA(((3 + len(rows_of)) * chips,))],
        compiler_params=room(8),
        name="pack",
    )(*in_hbm(queries, keys, values))


def stage_kernel(w_ref, out, arrived):
    copy = pltpu.make_async_copy(w_ref, out, arrived.at[0])
    copy.start()
    copy.wait()


def stage(weight):
    return pl.pallas_call(
        stage_kernel,
        out_shape=pltpu.VMEM(weight.shape, weight.dtype),
        in_specs=[pl.BlockSpec(memory_space=pltpu.HBM)],
        scratch_shapes=[pltpu.SemaphoreType.DMA((1,))],
        compiler_params=room(4),
        name="stage",
    )(*in_hbm(weight))


def attend_rows(q_part, k_all, v_all, o_all, rows_from, core, chips, heads):
    length, wide_k = k_all.shape[0] // (2 * chips), heads * KD
    count = o_all.shape[0] // chips
    reach = length + rows_from + count
    row = lax.broadcasted_iota(jnp.int32, (count, reach), 0) + (core * length + rows_from)
    seen = lax.broadcasted_iota(jnp.int32, (count, reach), 1) <= row
    seen = jnp.concatenate([seen] * heads, axis=0)
    lane = lax.broadcasted_iota(jnp.int32, (count, wide_k), 1) // KD
    for index in range(chips):
        q = q_part[index * count : (index + 1) * count, :] * jnp.bfloat16(KD ** (-0.5))
        stacked = jnp.concatenate([jnp.where(lane == head, q, jnp.bfloat16(0)) for head in range(heads)], axis=0)
        total = denominator = None
        for block in range(index + 1):
            at = 2 * block * length
            rows = slice(at, at + (reach if block == index else 2 * length))
            scores = lax.dot_general(
                stacked, k_all[rows, :], (((1,), (1,)), ((), ())), preferred_element_type=jnp.float32
            )
            raised = scores + 1.0
            weights = raised * raised + 1.0
            if block == index:
                weights = jnp.where(seen, weights, 0.0)
            weights = weights.astype(jnp.bfloat16)
            part = jnp.dot(weights, v_all[rows, :], preferred_element_type=jnp.float32)
            total = part if total is None else total + part
            sums = jnp.sum(weights.astype(jnp.float32), axis=1, keepdims=True)
            denominator = sums if denominator is None else denominator + sums
        for head in range(heads):
            own = slice(head * count, (head + 1) * count)
            lanes = slice(head * VD, (head + 1) * VD)
            o_all[index * count : (index + 1) * count, lanes] = (total[own, lanes] / denominator[own]).astype(
                jnp.bfloat16
            )


def deal(o_all, outs, chip):
    count = outs[0].shape[0]
    for turn, out in enumerate(outs):
        out[...] = o_all[pl.ds(pl.multiple_of((chip ^ turn) * count, count), count), :]


def attend_first_kernel(*refs, chips, heads):
    mine, partner = refs[:chips], refs[chips : 2 * chips]
    outs, (k_all, v_all) = refs[2 * chips : 3 * chips], refs[3 * chips : 3 * chips + 2]
    q_part, o_all = refs[-2:]
    wide_k = heads * KD
    length, count = k_all.shape[0] // (2 * chips), q_part.shape[0] // chips
    _, rows_of = stacks(count, mine[0].shape[1] // wide_k)
    chip, core = seat()
    for turn in range(chips):
        there = chip ^ turn
        for tile, (at, size) in enumerate(rows_of):
            q_part[pl.ds(pl.multiple_of(there * count + at, 16), size), :] = mine[turn][
                length : length + size, tile * wide_k : (tile + 1) * wide_k
            ]
        for ref, side in ((mine[turn], core), (partner[turn], 1 - core)):
            rows = pl.ds(pl.multiple_of((2 * there + side) * length, length), length)
            k_all[rows, :] = ref[:length, :wide_k]
            v_all[rows, :] = ref[:length, wide_k:]
    attend_rows(q_part, k_all, v_all, o_all, 0, core, chips, heads)
    deal(o_all, outs, chip)


def attend_later_kernel(k_all, v_all, *refs, chips, heads, rows_from):
    queries, outs, (q_part, o_all) = refs[:chips], refs[chips : 2 * chips], refs[2 * chips :]
    count = q_part.shape[0] // chips
    chip, core = seat()
    for turn in range(chips):
        q_part[pl.ds(pl.multiple_of((chip ^ turn) * count, count), count), :] = queries[turn][...]
    attend_rows(q_part, k_all, v_all, o_all, rows_from, core, chips, heads)
    deal(o_all, outs, chip)


def attend(mine, partner, later, heads, cuts):
    chips, length, kind = len(mine), cuts[-1], mine[0].dtype
    whole, (first, second) = 2 * chips * length, (cuts[1], cuts[2] - cuts[1])

    def scratch(size):
        return [pltpu.VMEM((chips * size, heads * KD), kind), pltpu.VMEM((chips * size, heads * VD), kind)]

    *one, k_all, v_all = pl.pallas_call(
        functools.partial(attend_first_kernel, chips=chips, heads=heads),
        out_shape=(
            *(pltpu.VMEM((first, heads * VD), kind),) * chips,
            pltpu.VMEM((whole, heads * KD), kind),
            pltpu.VMEM((whole, heads * VD), kind),
        ),
        scratch_shapes=scratch(first),
        compiler_params=room(20),
        name="attend0",
    )(*in_vmem(*mine, *partner))
    other = pl.pallas_call(
        functools.partial(attend_later_kernel, chips=chips, heads=heads, rows_from=first),
        out_shape=(pltpu.VMEM((second, heads * VD), kind),) * chips,
        scratch_shapes=scratch(second),
        compiler_params=room(16),
        name="attend1",
    )(*in_vmem(k_all, v_all, *later))
    return [one, other]


def block_at(slot):
    rank = lax.axis_index("head")
    turns = [(3, 3, 0, 0), (2, 2, 1, 1), (1, 0, 3, 2), (0, 1, 2, 3), (2, 0, 3, 1)][slot]
    block = jnp.int32(turns[0])
    for other in range(1, 4):
        block = jnp.where(rank == other, jnp.int32(turns[other]), block)
    return block


def project_kernel(*refs, chips, chunks, jobs):
    pieces, w_ref, outs = refs[: chunks * chips], refs[chunks * chips], refs[chunks * chips + 1 :]
    depth, columns = pieces[0].shape[1], outs[0].shape[1]
    here, _ = seat()
    for (slot, wanted), out in zip(jobs, outs):
        at = pl.ds(pl.multiple_of(block_at(slot) * columns, columns), columns)
        low = 0
        for chunk in wanted:
            total = None
            for turn in range(chips):
                rows = pl.ds(pl.multiple_of((here ^ turn) * depth, depth), depth)
                part = jnp.dot(
                    pieces[chunk * chips + turn][...], w_ref[rows, at], preferred_element_type=jnp.float32
                )
                total = part if total is None else total + part
            out[low : low + total.shape[0], :] = total.astype(out.dtype)
            low += total.shape[0]


def project(chunks, weight, columns, jobs, kinds):
    sizes = [pieces[0].shape[0] for pieces in chunks]
    return pl.pallas_call(
        functools.partial(project_kernel, chips=len(chunks[0]), chunks=len(chunks), jobs=jobs),
        out_shape=tuple(
            pltpu.VMEM((sum(sizes[chunk] for chunk in wanted), columns), kind)
            for (_, wanted), kind in zip(jobs, kinds)
        ),
        compiler_params=room(12),
    )(*in_vmem(*(piece for pieces in chunks for piece in pieces), weight))


def join_kernel(one, other, out, *, low):
    rows = one[low : low + other.shape[0], :].astype(jnp.float32)
    out[...] = (rows + other[...].astype(jnp.float32)).astype(out.dtype)


def join(one, other, low):
    return pl.pallas_call(
        functools.partial(join_kernel, low=low),
        out_shape=pltpu.VMEM(other.shape, other.dtype),
        compiler_params=room(4),
        name="join",
    )(*in_vmem(one, other))


def finish_kernel(own, third, *refs, cuts, arrivals):
    out, rows, sent = refs[-3:]
    rank = lax.axis_index("head")
    edge = (rank == 0) | (rank == 3)
    copies, at = [], 0
    for low, high, count in zip(cuts, cuts[1:], arrivals):
        total = own[low:high, :] + third[low:high, :].astype(jnp.float32)
        for part in refs[at : at + min(count, 2)]:
            total = total + part[...].astype(jnp.float32)
        if count == 3:
            beside = refs[at + 2][...].astype(jnp.float32)
            total = total + jnp.where(edge, beside, jnp.zeros_like(beside))
        at += count
        rows[low:high, :] = total.astype(rows.dtype)
        copies.append(
            pltpu.make_async_copy(rows.at[low:high, :], out.at[low:high, :], sent.at[len(copies)])
        )
        copies[-1].start()
    for copy in copies:
        copy.wait()


def finish(own, third, parts, cuts):
    flat = [part for some in parts for part in some]
    return pl.pallas_call(
        functools.partial(finish_kernel, cuts=cuts, arrivals=tuple(len(some) for some in parts)),
        out_shape=jax.ShapeDtypeStruct(own.shape, third.dtype),
        in_specs=[pl.BlockSpec(memory_space=pltpu.VMEM)] * (2 + len(flat)),
        out_specs=pl.BlockSpec(memory_space=pltpu.HBM),
        scratch_shapes=[pltpu.VMEM(own.shape, third.dtype), pltpu.SemaphoreType.DMA((len(parts),))],
        compiler_params=room(8),
        name="finish",
    )(*in_vmem(own, third, *flat))


def exchanged(queries, key_vectors, value_vectors, out_weight):
    seq, ranks = lax.axis_size("seq"), lax.axis_size("head")
    chips = seq // 2
    heads = out_weight.shape[0] // VD // chips
    columns = out_weight.shape[1] // ranks
    length = queries.shape[0]
    cuts = (0, length // 2, length)
    bf16, f32 = jnp.bfloat16, jnp.float32

    packed = pack(queries, key_vectors, value_vectors, chips, cuts[1])
    packed, later = packed[:chips], packed[chips:]
    mine = [packed[0]] + [swap(packed[turn], "seq", 2 * turn) for turn in range(1, chips)]
    partner = [swap(piece, "seq", 1) for piece in mine]
    later = [later[0]] + [swap(later[turn], "seq", 2 * turn) for turn in range(1, chips)]
    results = attend(mine, partner, later, heads, cuts)
    weight = stage(out_weight)
    chunks = [[outs[0]] + [swap(outs[turn], "seq", 2 * turn) for turn in range(1, chips)] for outs in results]

    def hop(value, source, target):
        pairs = [(source, target), (ranks - 1 - source, ranks - 1 - target)]
        return lax.ppermute(value, "head", pairs)

    to_first, to_second = [None, None], [None, None]
    (to_first[0],) = project(chunks[:1], weight, columns, ((0, (0,)),), (bf16,))
    (to_second[0],) = project(chunks[:1], weight, columns, ((1, (0,)),), (bf16,))
    (to_first[1],) = project(chunks[1:], weight, columns, ((0, (0,)),), (bf16,))
    both_ways, to_second[1], to_third, own = project(
        chunks, weight, columns, ((4, (1,)), (1, (1,)), (2, (0, 1)), (3, (0, 1))), (bf16, bf16, bf16, f32)
    )
    first = [hop(value, 0, 1) for value in to_first]
    second = [hop(to_second[0], 0, 1)]
    second.append(lax.ppermute(both_ways, "head", [(0, 1), (1, 0), (2, 3), (3, 2)]))
    third = hop(to_third, 0, 1)
    joined = [join(mine, other, 0) for mine, other in zip(to_first, first)]
    late = [hop(join(mine, other, 0), 1, 2) for mine, other in zip(to_second, second)]
    last = hop(join(to_third, hop(joined[0], 1, 2), 0), 2, 3)
    straight = hop(joined[1], 1, 3)
    return finish(own, third, ((late[0], last), (late[1], straight, second[1])), cuts)


def gathered(queries, key_vectors, value_vectors, out_weight):
    heads_here = out_weight.shape[0] // VD
    length = queries.shape[0]
    here = lax.axis_index("seq")
    k_all = lax.all_gather(key_vectors, "seq", axis=0, tiled=True)
    v_all = lax.all_gather(value_vectors, "seq", axis=0, tiled=True)
    rows = here * length + jnp.arange(length, dtype=jnp.int32)
    causal = jnp.arange(k_all.shape[0], dtype=jnp.int32)[None, :] <= rows[:, None]
    results = []
    for head in range(heads_here):
        q = queries[:, head * KD : (head + 1) * KD]
        k = k_all[:, head * KD : (head + 1) * KD]
        v = v_all[:, head * VD : (head + 1) * VD]
        scores = jnp.einsum("bd,td->bt", q, k, preferred_element_type=jnp.float32) * KD ** (-0.5)
        weights = jnp.where(causal, 1.0 + scores + 0.5 * scores * scores, 0.0).astype(jnp.bfloat16)
        numer = jnp.dot(weights, v, preferred_element_type=jnp.float32)
        denom = jnp.sum(weights, axis=-1, dtype=jnp.float32)
        results.append((numer / denom[:, None]).astype(jnp.bfloat16))
    attention = jnp.concatenate(results, axis=1)
    partial = jnp.dot(attention, out_weight, preferred_element_type=jnp.float32)
    mixed = lax.psum_scatter(partial, "head", scatter_dimension=1, tiled=True)
    return mixed.astype(jnp.bfloat16)


def planned(seq, ranks, heads_here):
    chips = seq // 2
    paired = seq == 2 * chips and chips > 0 and chips & (chips - 1) == 0
    return paired and ranks == 4 and heads_here % chips == 0 and (heads_here // chips * KD) % 128 == 0


def per_device(queries, key_vectors, value_vectors, out_weight):
    if planned(lax.axis_size("seq"), lax.axis_size("head"), out_weight.shape[0] // VD):
        return exchanged(queries, key_vectors, value_vectors, out_weight)
    return gathered(queries, key_vectors, value_vectors, out_weight)


def solution(mesh):
    placed = (P("seq", "head"), P("seq", "head"), P("seq", "head"), P("head", None))
    step = jax.shard_map(
        per_device, mesh=mesh, in_specs=placed, out_specs=P("seq", "head"), check_vma=False
    )
    seq, ranks = mesh.shape["seq"], mesh.shape["head"]

    def whole(queries, key_vectors, value_vectors, out_weight):
        run = step
        if planned(seq, ranks, out_weight.shape[0] // ranks // VD):
            run = step
        return run(queries, key_vectors, value_vectors, out_weight)

    return whole
```
